32 devices in a mesh: dp: 4 (over z), blk: 4 (over y, core), aa: 2 (over x).
Axes of the slice: x: 2, y: 2, z: 4, core: 2. Of those that a mesh axis runs over, the one named last changes fastest.
Arguments:
- queries: bfloat16 [4, 1024, 2048], P('dp', ('blk', 'aa')), may hold values from -128 to 128
- keys: bfloat16 [4, 1024, 512], P('dp', ('blk', 'aa')), may hold values from -10 to 10
- values: bfloat16 [4, 1024, 512], P('dp', ('blk', 'aa')), may hold values from -6 to 6
- grad_parts: float32 [4, 8, 131072], P('dp', ('blk', 'aa')), may hold values from -192 to 192
Outputs:
- attended: bfloat16 [4, 1024, 2048], P('dp', 'blk', 'aa')
- grad_mean: float32 [131072], P(('blk', 'aa'))
The draws below stay inside these ranges and needn't reach their ends.
All inputs are finite; a program needn't handle non-finite values.
Results may differ from the reference program's by a relative error of at most 0.008.
Values may be sent and summed in bfloat16 or wider, within the bound.
A program may use at most 64 MiB of HBM per device.

```python
import jax
import jax.numpy as jnp
from jax import lax

HQ = 16
KVH = 4
DH = 128
TOK_DEV = 128
BUCKET = 131072
SEQ = 1024
N_DP = 4
N_BLK = 4
N_AA = 2


def draw_keys(key, part):
    total_rows = TOK_DEV * N_BLK * N_AA
    drawn = jnp.clip(jax.random.normal(jax.random.fold_in(key, 21), (N_DP, total_rows, KVH * DH), jnp.float32), -6.0, 6.0)
    return drawn.astype(jnp.bfloat16)


def draw_queries(key, part):
    total_rows = TOK_DEV * N_BLK * N_AA
    drawn = jnp.clip(jax.random.normal(jax.random.fold_in(key, 31), (N_DP, total_rows, HQ * DH), jnp.float32), -6.0, 6.0)
    return drawn.astype(jnp.bfloat16)


def raised(drawn, key, source, target, shards_of, factor):
    def block_of(dim):
        return (jnp.arange(drawn.shape[dim]) // (drawn.shape[dim] // shards_of)).reshape((-1,) + (1,) * (drawn.ndim - 1 - dim))

    first = jax.random.permutation(key, shards_of)[block_of(target)]
    other_side = (block_of(target) + shards_of // 2) % shards_of
    return jnp.where((block_of(source) == first) | (block_of(source) == other_side), factor * drawn, drawn)


def level_of(own_key, dims, shards, least, largest):
    gain, own = 1.0, jax.random.fold_in(own_key, 6)
    for axis_at, parts in shards:
        draws = jnp.exp(jax.random.uniform(jax.random.fold_in(own, axis_at), (parts,), jnp.float32, least / len(shards), largest / len(shards)))
        gain = gain * jnp.repeat(draws, dims[axis_at] // parts).reshape([-1 if axis == axis_at else 1 for axis in range(len(dims))])
    return gain


def centred(key, extent, deviation, bound, cuts=(), held_as=jnp.bfloat16):
    factor_of = level_of(key, extent, cuts, -0.22, 0.18) if cuts else 1.0
    entries = jax.random.normal(key, extent, jnp.float32) * deviation * factor_of
    return jnp.minimum(jnp.maximum(entries, -bound), bound).astype(held_as)


def heavy_noise(key, dims, scale, most, shards, heavy, held_as=jnp.bfloat16):
    array = scale * jax.random.normal(key, dims, jnp.float32)
    if shards:
        array = array * level_of(key, dims, shards, -0.22, 0.18)
    return jnp.clip(raised(array, jax.random.fold_in(key, 3), *heavy), -most, most).astype(held_as)


def setup_inputs(seed: int = 0) -> dict:
    seeds = jax.random.split(jax.random.key(seed), 5)
    return {
        "queries": draw_queries(jax.random.fold_in(seeds[4], 71), 0),
        "keys": draw_keys(jax.random.fold_in(seeds[4], 71), 0),
        "values": centred(seeds[2], (N_DP, SEQ, KVH * DH), 1.0, 6.0, ((0, 4), (1, 8))),
        "grad_parts": heavy_noise(seeds[3], (N_DP, N_BLK * N_AA, BUCKET), 32.0, 192.0, ((0, 4), (1, 8)), (1, 2, 8, 2.0), jnp.float32),
    }


def attend_one(q_rep, k_rep, v_rep):
    total_rows = q_rep.shape[0]
    reach = total_rows // (4 * N_BLK)
    step_rows = min(256, reach)
    group = HQ // KVH
    q_heads = q_rep.reshape(total_rows, HQ, DH)
    pad_zero = jnp.zeros((reach, KVH, DH), jnp.bfloat16)
    k_padded = jnp.concatenate([pad_zero, k_rep.reshape(total_rows, KVH, DH)], 0)
    v_padded = jnp.concatenate([pad_zero, v_rep.reshape(total_rows, KVH, DH)], 0)
    scale = DH ** -0.5

    def one_block(index):
        start = (index * step_rows).astype(jnp.int32)
        q_block = lax.dynamic_slice_in_dim(q_heads, start, step_rows, 0).astype(jnp.float32)
        k_block = jnp.repeat(lax.dynamic_slice_in_dim(k_padded, start, step_rows + reach, 0), group, axis=1).astype(jnp.float32)
        v_block = jnp.repeat(lax.dynamic_slice_in_dim(v_padded, start, step_rows + reach, 0), group, axis=1).astype(jnp.float32)
        scores = jnp.einsum("qhd,khd->hqk", q_block, k_block) * scale
        q_pos = start + jnp.arange(step_rows, dtype=jnp.int32)
        k_pos = start - reach + jnp.arange(step_rows + reach, dtype=jnp.int32)
        allowed = (k_pos[None, :] <= q_pos[:, None]) & (k_pos[None, :] > q_pos[:, None] - reach)
        scores = jnp.where(allowed[None], scores, -1e30)
        top = jnp.max(scores, axis=-1, keepdims=True)
        expo = jnp.exp(scores - top)
        weights = (expo / jnp.sum(expo, axis=-1, keepdims=True)).astype(jnp.bfloat16)
        out = jnp.einsum("hqk,khd->qhd", weights.astype(jnp.float32), v_block)
        return out.astype(jnp.bfloat16)

    blocks = lax.map(one_block, jnp.arange(total_rows // step_rows, dtype=jnp.int32))
    return blocks.reshape(total_rows, HQ * DH)


def reference(queries, keys, values, grad_parts):
    def one_replica(triple):
        return attend_one(triple[0], triple[1], triple[2])

    attended = lax.map(one_replica, (queries, keys, values))
    count = grad_parts.shape[0] * grad_parts.shape[1]
    grad_mean = jnp.sum(grad_parts.astype(jnp.float32), axis=(0, 1)) / count
    return attended, grad_mean
```

```python
import functools

import jax
import jax.numpy as jnp
from jax import lax
from jax.experimental import pallas as pl
from jax.experimental.pallas import tpu as pltpu
from jax.sharding import PartitionSpec as P

HQ = 16
KVH = 4
DH = 128
LANES = 128
MESH = pl.DeviceIdType.MESH


def shifted(value, axis, by):
    peers = lax.axis_size(axis)
    pairs = [(i, i + by) for i in range(peers) if 0 <= i + by < peers]
    return lax.ppermute(value, axis, pairs)


def attend(queries, keys, values):
    rows = queries.shape[0]
    size_aa = lax.axis_size("aa")
    spread = max(KVH, size_aa)
    q_heads = queries.reshape(rows, HQ, DH)
    k_heads = jnp.repeat(keys.reshape(rows, KVH, DH), spread // KVH, axis=1)
    v_heads = jnp.repeat(values.reshape(rows, KVH, DH), spread // KVH, axis=1)
    q_here, k_here, v_here = (
        lax.all_to_all(q_heads, "aa", split_axis=1, concat_axis=0, tiled=True),
        lax.all_to_all(k_heads, "aa", split_axis=1, concat_axis=0, tiled=True),
        lax.all_to_all(v_heads, "aa", split_axis=1, concat_axis=0, tiled=True),
    )
    span = q_here.shape[0]
    reach = span // 4
    prior_k, prior_v = shifted((k_here[span - reach :], v_here[span - reach :]), "blk", 1)
    group = q_here.shape[1] // k_here.shape[1]
    k_all = jnp.repeat(jnp.concatenate([prior_k, k_here], 0), group, axis=1)
    v_all = jnp.repeat(jnp.concatenate([prior_v, v_here], 0), group, axis=1)
    step_rows = min(256, reach)
    anchor = lax.axis_index("blk") * span
    scale = DH ** (-0.5)

    def one_block(index):
        offset = index * step_rows
        q_block = lax.dynamic_slice_in_dim(q_here, offset, step_rows, 0)
        k_block = lax.dynamic_slice_in_dim(k_all, offset, step_rows + reach, 0)
        v_block = lax.dynamic_slice_in_dim(v_all, offset, step_rows + reach, 0)
        scores = (
            jnp.einsum("qhd,khd->hqk", q_block, k_block, preferred_element_type=jnp.float32) * scale
        )
        q_pos = anchor + offset + jnp.arange(step_rows, dtype=jnp.int32)
        k_pos = anchor + offset - reach + jnp.arange(step_rows + reach, dtype=jnp.int32)
        allowed = (k_pos[None, :] <= q_pos[:, None]) & (k_pos[None, :] > q_pos[:, None] - reach)
        scores = jnp.where(allowed[None], scores, -1e30)
        top = jnp.max(scores, axis=-1, keepdims=True)
        expo = jnp.exp(scores - top)
        weights = (expo / jnp.sum(expo, axis=-1, keepdims=True)).astype(jnp.bfloat16)
        out = jnp.einsum("hqk,khd->qhd", weights, v_block, preferred_element_type=jnp.float32)
        return out.astype(jnp.bfloat16)

    blocks = lax.map(one_block, jnp.arange(span // step_rows, dtype=jnp.int32))
    return blocks.reshape(span, -1)


def average(grad_parts):
    members = lax.axis_size("blk") * lax.axis_size("aa")
    replicas = lax.axis_size("dp")
    flat_grad = grad_parts.reshape(-1)
    share = lax.psum_scatter(flat_grad, ("blk", "aa"), scatter_dimension=0, tiled=True)
    total = lax.psum(share, "dp")
    return total / (members * replicas)


def shards(queries, keys, values, grad_parts):
    attended = attend(queries[0], keys[0], values[0])[None]
    grad_mean = average(grad_parts)
    return (attended, grad_mean)


def fused_kernel(
    sizes, q_hbm, k_hbm, v_hbm, g_hbm, out_ref, mean_ref,
    q_ref, k_ref, v_ref, g_ref, o_send, o_own, m_own, g1_send, g1_recv, g2_send, g2_recv, g3,
    load_sem, halo_send, halo_recv, o_send_sem, o_recv_sem, own_sem,
    g1_sem, g2_send_sem, g2_recv_sem, g3_send_sem, g3_recv_sem,
):
    n_dp, n_blk, n_aa = sizes
    tok = q_hbm.shape[0]
    reach = tok // 2
    group = HQ // KVH
    kv_here = KVH // n_aa
    wide = group * DH
    n_y = n_blk // 2
    plane = n_y * n_aa
    share = g2_send.shape[1]
    dp, blk, aa = lax.axis_index("dp"), lax.axis_index("blk"), lax.axis_index("aa")
    core, y = blk % 2, blk // 2
    other = 1 - aa
    place = blk * n_aa + aa
    last = n_blk * n_aa - 1
    spot = y * n_aa + aa

    loads = [
        pltpu.make_async_copy(k_hbm, k_ref.at[pl.ds(reach, tok)], load_sem.at[0]),
        pltpu.make_async_copy(v_hbm, v_ref.at[pl.ds(reach, tok)], load_sem.at[1]),
        pltpu.make_async_copy(g_hbm, g_ref, load_sem.at[2]),
        pltpu.make_async_copy(q_hbm, q_ref, load_sem.at[3]),
    ]
    for load in loads:
        load.start()

    partner = (dp, blk + 1 - 2 * core, aa)

    def plane_peer(d):
        to = (spot + d) % plane
        return to, (dp, (to // n_aa) * 2 + core, to % n_aa)

    def dp_peer(d):
        return ((dp + d) % n_dp, blk, aa)

    def at_place(p):
        return (dp, p // n_aa, p % n_aa)

    barrier = pltpu.get_barrier_semaphore()
    greeted = [partner] + [plane_peer(d)[1] for d in range(1, plane)]
    greeted += [dp_peer(d) for d in range(1, n_dp)]
    for peer in greeted:
        pl.semaphore_signal(barrier, inc=1, device_id=peer, device_id_type=MESH)
    ahead = (aa == n_aa - 1) & (place < last)
    behind = (aa == 0) & (place > 0)

    @pl.when(ahead)
    def _():
        pl.semaphore_signal(barrier, inc=1, device_id=at_place(place + 1), device_id_type=MESH)

    @pl.when(behind)
    def _():
        pl.semaphore_signal(barrier, inc=1, device_id=at_place(place - 1), device_id_type=MESH)

    @pl.when(place == 0)
    def _():
        k_ref[0:reach] = jnp.zeros((reach, KVH * DH), k_ref.dtype)
        v_ref[0:reach] = jnp.zeros((reach, KVH * DH), v_ref.dtype)

    def rows_of(y_at, core_at):
        return pl.ds(pl.multiple_of((y_at * 2 + core_at) * n_aa * share, share), n_aa * share)

    loads[2].wait()
    for y_at in range(n_y):
        g1_send[y_at] = g_ref[rows_of(y_at, 1 - core)].astype(jnp.bfloat16)
    loads[0].wait()
    loads[1].wait()

    @pl.when(ahead | behind)
    def _():
        pl.semaphore_wait(barrier, len(greeted) + 1)

    @pl.when(jnp.logical_not(ahead | behind))
    def _():
        pl.semaphore_wait(barrier, len(greeted))

    def remote(src, dst, send_sem, recv_sem, to):
        return pltpu.make_async_remote_copy(
            src_ref=src, dst_ref=dst, send_sem=send_sem, recv_sem=recv_sem,
            device_id=to, device_id_type=MESH,
        )

    first = remote(g1_send, g1_recv, g1_sem.at[0], g1_sem.at[1], partner)
    first.start()

    def halo(ref, i):
        return remote(
            ref.at[pl.ds(tok, reach)], ref.at[pl.ds(0, reach)],
            halo_send.at[i], halo_recv.at[i], at_place(jnp.minimum(place + 1, last)),
        )

    @pl.when(place < last)
    def _():
        halo(k_ref, 0).start()
        halo(v_ref, 1).start()

    def unit(block, kv, target):
        kv_at = target * kv_here + kv
        rows = pl.ds(block * reach, reach)
        span = pl.ds(block * reach, 2 * reach)
        q_cols = pl.multiple_of(kv_at * wide, wide)
        kv_cols = pl.ds(pl.multiple_of(kv_at * DH, DH), DH)
        q_all = q_ref[rows, pl.ds(q_cols, wide)]
        q = jnp.concatenate([q_all[:, h * DH : (h + 1) * DH] for h in range(group)], 0)
        scores = lax.dot_general(
            q, k_ref[span, kv_cols], (((1,), (1,)), ((), ())), preferred_element_type=jnp.float32
        ) * (DH ** -0.5)
        i = lax.broadcasted_iota(jnp.int32, scores.shape, 0) % reach
        j = lax.broadcasted_iota(jnp.int32, scores.shape, 1)
        scores = jnp.where((j > i) & (j <= i + reach), scores, -1e30)
        expo = jnp.exp(scores - jnp.max(scores, axis=-1, keepdims=True))
        weights = (expo / jnp.sum(expo, axis=-1, keepdims=True)).astype(jnp.bfloat16)
        out = jnp.dot(weights, v_ref[span, kv_cols], preferred_element_type=jnp.float32)
        out = out.astype(jnp.bfloat16)
        return jnp.concatenate([out[h * reach : (h + 1) * reach] for h in range(group)], 1)

    def send_out(block, kv):
        cols = pl.ds(kv * wide, wide)
        start = pl.multiple_of(aa * tok + block * reach, reach)
        at = block * kv_here + kv
        return remote(
            o_send.at[pl.ds(block * reach, reach), cols], out_ref.at[pl.ds(start, reach), cols],
            o_send_sem.at[at], o_recv_sem.at[at], (dp, blk, other),
        )

    def for_other(block):
        for kv in range(kv_here):
            o_send[pl.ds(block * reach, reach), pl.ds(kv * wide, wide)] = unit(block, kv, other)

    def for_self(block):
        for kv in range(kv_here):
            o_own[pl.ds(block * reach, reach), pl.ds(kv * wide, wide)] = unit(block, kv, aa)

    loads[3].wait()
    for_other(1)

    first.wait_recv()
    for y_at in range(n_y):
        summed = g_ref[rows_of(y_at, core)] + g1_recv[y_at].astype(jnp.float32)
        for a_at in range(n_aa):
            g2_send[y_at * n_aa + a_at] = summed[a_at * share : (a_at + 1) * share].astype(jnp.bfloat16)

    def second(d):
        to, peer = plane_peer(d)
        return remote(
            g2_send.at[to], g2_recv.at[d - 1], g2_send_sem.at[d - 1], g2_recv_sem.at[d - 1], peer
        )

    for d in range(1, plane):
        second(d).start()
    for kv in range(kv_here):
        send_out(1, kv).start()
    for_self(1)

    @pl.when(place > 0)
    def _():
        halo(k_ref, 0).wait_recv()
        halo(v_ref, 1).wait_recv()

    for_other(0)
    for kv in range(kv_here):
        send_out(0, kv).start()

    own_rows = pl.ds(pl.multiple_of(place * share, share), share)
    own = g_ref[own_rows] + g1_recv[y, pl.ds(pl.multiple_of(aa * share, share), share)].astype(jnp.float32)
    for d in range(1, plane):
        second(d).wait_recv()
        own = own + g2_recv[d - 1].astype(jnp.float32)
    g3[dp] = own.astype(jnp.bfloat16)

    def third(d):
        return remote(
            g3.at[dp], g3.at[dp], g3_send_sem.at[d - 1], g3_recv_sem.at[d - 1], dp_peer(d)
        )

    def third_in(d):
        origin = (dp + n_dp - d) % n_dp
        return remote(
            g3.at[origin], g3.at[origin], g3_send_sem.at[d - 1], g3_recv_sem.at[d - 1], dp_peer(d)
        )

    for d in range(1, n_dp):
        third(d).start()

    for_self(0)
    own_out = pltpu.make_async_copy(
        o_own, out_ref.at[pl.ds(pl.multiple_of(aa * tok, tok), tok)], own_sem.at[0]
    )
    own_out.start()

    for d in range(1, n_dp):
        third_in(d).wait_recv()
    total = g3[0].astype(jnp.float32)
    for z in range(1, n_dp):
        total = total + g3[z].astype(jnp.float32)
    m_own[...] = total / (n_dp * n_blk * n_aa)
    mean_out = pltpu.make_async_copy(m_own, mean_ref, own_sem.at[1])
    mean_out.start()

    first.wait_send()

    @pl.when(place < last)
    def _():
        halo(k_ref, 0).wait_send()
        halo(v_ref, 1).wait_send()

    for d in range(1, plane):
        second(d).wait_send()
    for d in range(1, n_dp):
        third(d).wait_send()
    for block in (1, 0):
        for kv in range(kv_here):
            send_out(block, kv).wait()
    own_out.wait()
    mean_out.wait()


def fused(sizes, queries, keys, values, grad_parts):
    n_dp, n_blk, n_aa = sizes
    tok, q_width = queries.shape[1:]
    reach = tok // 2
    rows = grad_parts.size // LANES
    share = rows // (n_blk * n_aa)
    plane = n_blk // 2 * n_aa
    kv_here = KVH // n_aa
    bf16, f32 = jnp.bfloat16, jnp.float32
    dma = lambda *shape: pltpu.SemaphoreType.DMA(shape)
    hbm = pl.BlockSpec(memory_space=pl.ANY)
    attended, mean = pl.pallas_call(
        functools.partial(fused_kernel, sizes),
        out_shape=(
            jax.ShapeDtypeStruct((tok * n_aa, q_width // n_aa), bf16),
            jax.ShapeDtypeStruct((share, LANES), f32),
        ),
        in_specs=[hbm] * 4,
        out_specs=(hbm, hbm),
        scratch_shapes=[
            pltpu.VMEM((tok, q_width), bf16),
            pltpu.VMEM((reach + tok, KVH * DH), bf16),
            pltpu.VMEM((reach + tok, KVH * DH), bf16),
            pltpu.VMEM((rows, LANES), f32),
            pltpu.VMEM((tok, q_width // n_aa), bf16),
            pltpu.VMEM((tok, q_width // n_aa), bf16),
            pltpu.VMEM((share, LANES), f32),
            pltpu.VMEM((n_blk // 2, n_aa * share, LANES), bf16),
            pltpu.VMEM((n_blk // 2, n_aa * share, LANES), bf16),
            pltpu.VMEM((plane, share, LANES), bf16),
            pltpu.VMEM((plane - 1, share, LANES), bf16),
            pltpu.VMEM((n_dp, share, LANES), bf16),
            dma(4), dma(2), dma(2), dma(2 * kv_here), dma(2 * kv_here), dma(2),
            dma(2), dma(plane - 1), dma(plane - 1), dma(n_dp - 1), dma(n_dp - 1),
        ],
        compiler_params=pltpu.CompilerParams(collective_id=0, has_side_effects=True),
        name="fused",
    )(queries[0], keys[0], values[0], grad_parts.reshape(rows, LANES))
    return attended[None], mean.reshape(-1)


def fits(sizes, args):
    n_dp, n_blk, n_aa = sizes
    queries, _, _, grad_parts = args
    rows, rest = divmod(grad_parts.shape[-1], LANES)
    shares = n_blk * n_aa
    tokens = queries.shape[1] // shares
    return (
        n_aa == 2 and n_blk % 2 == 0 and n_dp > 1 and KVH % n_aa == 0
        and tokens % 32 == 0 and rest == 0 and rows % (shares * 16) == 0
    )


def solution(mesh):
    placed = (
        P("dp", ("blk", "aa"), None),
        P("dp", ("blk", "aa"), None),
        P("dp", ("blk", "aa"), None),
        P("dp", ("blk", "aa"), None),
    )
    sizes = tuple(mesh.shape[axis] for axis in ("dp", "blk", "aa"))

    def step(*args):
        body = functools.partial(fused, sizes) if fits(sizes, args) else shards
        return jax.shard_map(
            body,
            mesh=mesh,
            in_specs=placed,
            out_specs=(P("dp", "blk", "aa"), P(("blk", "aa"))),
            check_vma=False,
        )(*args)

    return step
```

```python
import functools

import jax
import jax.numpy as jnp
from jax import lax
from jax.experimental import pallas as pl
from jax.experimental.pallas import tpu as pltpu
from jax.sharding import PartitionSpec as P

HQ = 16
KVH = 4
DH = 128
LANES = 128
MESH = pl.DeviceIdType.MESH


def shifted(value, axis, by):
    peers = lax.axis_size(axis)
    pairs = [(i, i + by) for i in range(peers) if 0 <= i + by < peers]
    return lax.ppermute(value, axis, pairs)


def attend(queries, keys, values):
    rows = queries.shape[0]
    size_aa = lax.axis_size("aa")
    spread = max(KVH, size_aa)
    q_heads = queries.reshape(rows, HQ, DH)
    k_heads = jnp.repeat(keys.reshape(rows, KVH, DH), spread // KVH, axis=1)
    v_heads = jnp.repeat(values.reshape(rows, KVH, DH), spread // KVH, axis=1)
    q_here, k_here, v_here = (
        lax.all_to_all(q_heads, "aa", split_axis=1, concat_axis=0, tiled=True),
        lax.all_to_all(k_heads, "aa", split_axis=1, concat_axis=0, tiled=True),
        lax.all_to_all(v_heads, "aa", split_axis=1, concat_axis=0, tiled=True),
    )
    span = q_here.shape[0]
    reach = span // 4
    prior_k, prior_v = shifted((k_here[span - reach :], v_here[span - reach :]), "blk", 1)
    group = q_here.shape[1] // k_here.shape[1]
    k_all = jnp.repeat(jnp.concatenate([prior_k, k_here], 0), group, axis=1)
    v_all = jnp.repeat(jnp.concatenate([prior_v, v_here], 0), group, axis=1)
    step_rows = min(256, reach)
    anchor = lax.axis_index("blk") * span
    scale = DH ** (-0.5)

    def one_block(index):
        offset = index * step_rows
        q_block = lax.dynamic_slice_in_dim(q_here, offset, step_rows, 0)
        k_block = lax.dynamic_slice_in_dim(k_all, offset, step_rows + reach, 0)
        v_block = lax.dynamic_slice_in_dim(v_all, offset, step_rows + reach, 0)
        scores = (
            jnp.einsum("qhd,khd->hqk", q_block, k_block, preferred_element_type=jnp.float32) * scale
        )
        q_pos = anchor + offset + jnp.arange(step_rows, dtype=jnp.int32)
        k_pos = anchor + offset - reach + jnp.arange(step_rows + reach, dtype=jnp.int32)
        allowed = (k_pos[None, :] <= q_pos[:, None]) & (k_pos[None, :] > q_pos[:, None] - reach)
        scores = jnp.where(allowed[None], scores, -1e30)
        top = jnp.max(scores, axis=-1, keepdims=True)
        expo = jnp.exp(scores - top)
        weights = (expo / jnp.sum(expo, axis=-1, keepdims=True)).astype(jnp.bfloat16)
        out = jnp.einsum("hqk,khd->qhd", weights, v_block, preferred_element_type=jnp.float32)
        return out.astype(jnp.bfloat16)

    blocks = lax.map(one_block, jnp.arange(span // step_rows, dtype=jnp.int32))
    return blocks.reshape(span, -1)


def average(grad_parts):
    members = lax.axis_size("blk") * lax.axis_size("aa")
    replicas = lax.axis_size("dp")
    flat_grad = grad_parts.reshape(-1)
    share = lax.psum_scatter(flat_grad, ("blk", "aa"), scatter_dimension=0, tiled=True)
    total = lax.psum(share, "dp")
    return total / (members * replicas)


def shards(queries, keys, values, grad_parts):
    attended = attend(queries[0], keys[0], values[0])[None]
    grad_mean = average(grad_parts)
    return (attended, grad_mean)


def fused_kernel(
    sizes, q_hbm, k_hbm, v_hbm, g_hbm, out_ref, mean_ref,
    q_ref, k_ref, v_ref, g_ref, o_send, g1_send, g1_recv, g2_send, g2_recv, g3,
    load_sem, halo_send, halo_recv, o_send_sem, o_recv_sem,
    g1_sem, g2_send_sem, g2_recv_sem, g3_send_sem, g3_recv_sem,
):
    n_dp, n_blk, n_aa = sizes
    tok = q_hbm.shape[0]
    reach = tok // 2
    group = HQ // KVH
    kv_here = KVH // n_aa
    wide = group * DH
    n_y = n_blk // 2
    plane = n_y * n_aa
    share = g2_send.shape[1]
    dp, blk, aa = lax.axis_index("dp"), lax.axis_index("blk"), lax.axis_index("aa")
    core, y = blk % 2, blk // 2
    other = 1 - aa
    place = blk * n_aa + aa
    last = n_blk * n_aa - 1
    spot = y * n_aa + aa

    loads = [
        pltpu.make_async_copy(k_hbm, k_ref.at[pl.ds(reach, tok)], load_sem.at[0]),
        pltpu.make_async_copy(v_hbm, v_ref.at[pl.ds(reach, tok)], load_sem.at[1]),
        pltpu.make_async_copy(g_hbm, g_ref, load_sem.at[2]),
        pltpu.make_async_copy(q_hbm, q_ref, load_sem.at[3]),
    ]
    for load in loads:
        load.start()

    partner = (dp, blk + 1 - 2 * core, aa)

    def plane_peer(d):
        to = (spot + d) % plane
        return to, (dp, (to // n_aa) * 2 + core, to % n_aa)

    def dp_peer(d):
        return ((dp + d) % n_dp, blk, aa)

    def at_place(p):
        return (dp, p // n_aa, p % n_aa)

    barrier = pltpu.get_barrier_semaphore()
    greeted = [partner] + [plane_peer(d)[1] for d in range(1, plane)]
    greeted += [dp_peer(d) for d in range(1, n_dp)]
    for peer in greeted:
        pl.semaphore_signal(barrier, inc=1, device_id=peer, device_id_type=MESH)
    ahead = (aa == n_aa - 1) & (place < last)
    behind = (aa == 0) & (place > 0)

    @pl.when(ahead)
    def _():
        pl.semaphore_signal(barrier, inc=1, device_id=at_place(place + 1), device_id_type=MESH)

    @pl.when(behind)
    def _():
        pl.semaphore_signal(barrier, inc=1, device_id=at_place(place - 1), device_id_type=MESH)

    @pl.when(place == 0)
    def _():
        k_ref[0:reach] = jnp.zeros((reach, KVH * DH), k_ref.dtype)
        v_ref[0:reach] = jnp.zeros((reach, KVH * DH), v_ref.dtype)

    def rows_of(y_at, core_at):
        return pl.ds(pl.multiple_of((y_at * 2 + core_at) * n_aa * share, share), n_aa * share)

    loads[2].wait()
    for y_at in range(n_y):
        g1_send[y_at] = g_ref[rows_of(y_at, 1 - core)].astype(jnp.bfloat16)
    loads[0].wait()
    loads[1].wait()

    @pl.when(ahead | behind)
    def _():
        pl.semaphore_wait(barrier, len(greeted) + 1)

    @pl.when(jnp.logical_not(ahead | behind))
    def _():
        pl.semaphore_wait(barrier, len(greeted))

    def remote(src, dst, send_sem, recv_sem, to):
        return pltpu.make_async_remote_copy(
            src_ref=src, dst_ref=dst, send_sem=send_sem, recv_sem=recv_sem,
            device_id=to, device_id_type=MESH,
        )

    first = remote(g1_send, g1_recv, g1_sem.at[0], g1_sem.at[1], partner)
    first.start()

    def halo(ref, i):
        return remote(
            ref.at[pl.ds(tok, reach)], ref.at[pl.ds(0, reach)],
            halo_send.at[i], halo_recv.at[i], at_place(jnp.minimum(place + 1, last)),
        )

    @pl.when(place < last)
    def _():
        halo(k_ref, 0).start()
        halo(v_ref, 1).start()

    def unit(block, kv, target):
        kv_at = target * kv_here + kv
        rows = pl.ds(block * reach, reach)
        span = pl.ds(block * reach, 2 * reach)
        q_cols = pl.multiple_of(kv_at * wide, wide)
        kv_cols = pl.ds(pl.multiple_of(kv_at * DH, DH), DH)
        q_all = q_ref[rows, pl.ds(q_cols, wide)]
        q = jnp.concatenate([q_all[:, h * DH : (h + 1) * DH] for h in range(group)], 0)
        scores = lax.dot_general(
            q, k_ref[span, kv_cols], (((1,), (1,)), ((), ())), preferred_element_type=jnp.float32
        ) * (DH ** -0.5)
        i = lax.broadcasted_iota(jnp.int32, scores.shape, 0) % reach
        j = lax.broadcasted_iota(jnp.int32, scores.shape, 1)
        scores = jnp.where((j > i) & (j <= i + reach), scores, -1e30)
        expo = jnp.exp(scores - jnp.max(scores, axis=-1, keepdims=True))
        weights = (expo / jnp.sum(expo, axis=-1, keepdims=True)).astype(jnp.bfloat16)
        out = jnp.dot(weights, v_ref[span, kv_cols], preferred_element_type=jnp.float32)
        out = out.astype(jnp.bfloat16)
        return jnp.concatenate([out[h * reach : (h + 1) * reach] for h in range(group)], 1)

    def send_out(block, kv):
        cols = pl.ds(kv * wide, wide)
        start = pl.multiple_of(aa * tok + block * reach, reach)
        at = block * kv_here + kv
        return remote(
            o_send.at[pl.ds(block * reach, reach), cols], out_ref.at[pl.ds(start, reach), cols],
            o_send_sem.at[at], o_recv_sem.at[at], (dp, blk, other),
        )

    def for_other(block):
        for kv in range(kv_here):
            o_send[pl.ds(block * reach, reach), pl.ds(kv * wide, wide)] = unit(block, kv, other)

    def for_self(block):
        for kv in range(kv_here):
            start = pl.multiple_of(aa * tok + block * reach, reach)
            out_ref[pl.ds(start, reach), pl.ds(kv * wide, wide)] = unit(block, kv, aa)

    loads[3].wait()
    for_other(1)

    first.wait_recv()
    for y_at in range(n_y):
        summed = g_ref[rows_of(y_at, core)] + g1_recv[y_at].astype(jnp.float32)
        for a_at in range(n_aa):
            g2_send[y_at * n_aa + a_at] = summed[a_at * share : (a_at + 1) * share].astype(jnp.bfloat16)

    def second(d):
        to, peer = plane_peer(d)
        return remote(
            g2_send.at[to], g2_recv.at[d - 1], g2_send_sem.at[d - 1], g2_recv_sem.at[d - 1], peer
        )

    for d in range(1, plane):
        second(d).start()
    for kv in range(kv_here):
        send_out(1, kv).start()
    for_self(1)

    @pl.when(place > 0)
    def _():
        halo(k_ref, 0).wait_recv()
        halo(v_ref, 1).wait_recv()

    for_other(0)
    for kv in range(kv_here):
        send_out(0, kv).start()

    own_rows = pl.ds(pl.multiple_of(place * share, share), share)
    own = g_ref[own_rows] + g1_recv[y, pl.ds(pl.multiple_of(aa * share, share), share)].astype(jnp.float32)
    for d in range(1, plane):
        second(d).wait_recv()
        own = own + g2_recv[d - 1].astype(jnp.float32)
    g3[dp] = own.astype(jnp.bfloat16)

    def third(d):
        return remote(
            g3.at[dp], g3.at[dp], g3_send_sem.at[d - 1], g3_recv_sem.at[d - 1], dp_peer(d)
        )

    def third_in(d):
        origin = (dp + n_dp - d) % n_dp
        return remote(
            g3.at[origin], g3.at[origin], g3_send_sem.at[d - 1], g3_recv_sem.at[d - 1], dp_peer(d)
        )

    for d in range(1, n_dp):
        third(d).start()

    for_self(0)
    for d in range(1, n_dp):
        third_in(d).wait_recv()
    total = g3[0].astype(jnp.float32)
    for z in range(1, n_dp):
        total = total + g3[z].astype(jnp.float32)
    mean_ref[...] = total / (n_dp * n_blk * n_aa)

    first.wait_send()

    @pl.when(place < last)
    def _():
        halo(k_ref, 0).wait_send()
        halo(v_ref, 1).wait_send()

    for d in range(1, plane):
        second(d).wait_send()
    for d in range(1, n_dp):
        third(d).wait_send()
    for block in (1, 0):
        for kv in range(kv_here):
            send_out(block, kv).wait()


def finish_kernel(out_in, mean_in, out_ref, mean_ref, sem):
    out_copy = pltpu.make_async_copy(out_in, out_ref, sem.at[0])
    mean_copy = pltpu.make_async_copy(mean_in, mean_ref, sem.at[1])
    out_copy.start()
    mean_copy.start()
    out_copy.wait()
    mean_copy.wait()


def fused(sizes, queries, keys, values, grad_parts):
    n_dp, n_blk, n_aa = sizes
    tok, q_width = queries.shape[1:]
    reach = tok // 2
    rows = grad_parts.size // LANES
    share = rows // (n_blk * n_aa)
    plane = n_blk // 2 * n_aa
    kv_here = KVH // n_aa
    bf16, f32 = jnp.bfloat16, jnp.float32
    dma = lambda *shape: pltpu.SemaphoreType.DMA(shape)
    vmem = pl.BlockSpec(memory_space=pltpu.VMEM)
    hbm = pl.BlockSpec(memory_space=pl.ANY)
    attended, mean = pl.pallas_call(
        functools.partial(fused_kernel, sizes),
        out_shape=(
            pltpu.VMEM((tok * n_aa, q_width // n_aa), bf16),
            pltpu.VMEM((share, LANES), f32),
        ),
        in_specs=[hbm] * 4,
        out_specs=(vmem, vmem),
        scratch_shapes=[
            pltpu.VMEM((tok, q_width), bf16),
            pltpu.VMEM((reach + tok, KVH * DH), bf16),
            pltpu.VMEM((reach + tok, KVH * DH), bf16),
            pltpu.VMEM((rows, LANES), f32),
            pltpu.VMEM((tok, q_width // n_aa), bf16),
            pltpu.VMEM((n_blk // 2, n_aa * share, LANES), bf16),
            pltpu.VMEM((n_blk // 2, n_aa * share, LANES), bf16),
            pltpu.VMEM((plane, share, LANES), bf16),
            pltpu.VMEM((plane - 1, share, LANES), bf16),
            pltpu.VMEM((n_dp, share, LANES), bf16),
            dma(4), dma(2), dma(2), dma(2 * kv_here), dma(2 * kv_here),
            dma(2), dma(plane - 1), dma(plane - 1), dma(n_dp - 1), dma(n_dp - 1),
        ],
        compiler_params=pltpu.CompilerParams(collective_id=0, has_side_effects=True),
        name="fused",
    )(queries[0], keys[0], values[0], grad_parts.reshape(rows, LANES))
    attended, mean = pl.pallas_call(
        finish_kernel,
        out_shape=tuple(jax.ShapeDtypeStruct(a.shape, a.dtype) for a in (attended, mean)),
        in_specs=[hbm] * 2,
        out_specs=(hbm, hbm),
        scratch_shapes=[dma(2)],
        compiler_params=pltpu.CompilerParams(vmem_limit_bytes=1024 * 1024),
        name="finish",
    )(attended, mean)
    return attended[None], mean.reshape(-1)


def fits(sizes, args):
    n_dp, n_blk, n_aa = sizes
    queries, _, _, grad_parts = args
    rows, rest = divmod(grad_parts.shape[-1], LANES)
    shares = n_blk * n_aa
    tokens = queries.shape[1] // shares
    return (
        n_aa == 2 and n_blk % 2 == 0 and n_dp > 1 and KVH % n_aa == 0
        and tokens % 32 == 0 and rest == 0 and rows % (shares * 16) == 0
    )


def solution(mesh):
    placed = (
        P("dp", ("blk", "aa"), None),
        P("dp", ("blk", "aa"), None),
        P("dp", ("blk", "aa"), None),
        P("dp", ("blk", "aa"), None),
    )
    sizes = tuple(mesh.shape[axis] for axis in ("dp", "blk", "aa"))

    def step(*args):
        body = functools.partial(fused, sizes) if fits(sizes, args) else shards
        return jax.shard_map(
            body,
            mesh=mesh,
            in_specs=placed,
            out_specs=(P("dp", "blk", "aa"), P(("blk", "aa"))),
            check_vma=False,
        )(*args)

    return step
```

```python
import functools

import jax
import jax.numpy as jnp
from jax import lax
from jax.experimental import pallas as pl
from jax.experimental.pallas import tpu as pltpu
from jax.sharding import PartitionSpec as P

HQ = 16
KVH = 4
DH = 128
LANES = 128
MESH = pl.DeviceIdType.MESH


def shifted(value, axis, by):
    peers = lax.axis_size(axis)
    pairs = [(i, i + by) for i in range(peers) if 0 <= i + by < peers]
    return lax.ppermute(value, axis, pairs)


def attend(queries, keys, values):
    rows = queries.shape[0]
    size_aa = lax.axis_size("aa")
    spread = max(KVH, size_aa)
    q_heads = queries.reshape(rows, HQ, DH)
    k_heads = jnp.repeat(keys.reshape(rows, KVH, DH), spread // KVH, axis=1)
    v_heads = jnp.repeat(values.reshape(rows, KVH, DH), spread // KVH, axis=1)
    q_here, k_here, v_here = (
        lax.all_to_all(q_heads, "aa", split_axis=1, concat_axis=0, tiled=True),
        lax.all_to_all(k_heads, "aa", split_axis=1, concat_axis=0, tiled=True),
        lax.all_to_all(v_heads, "aa", split_axis=1, concat_axis=0, tiled=True),
    )
    span = q_here.shape[0]
    reach = span // 4
    prior_k, prior_v = shifted((k_here[span - reach :], v_here[span - reach :]), "blk", 1)
    group = q_here.shape[1] // k_here.shape[1]
    k_all = jnp.repeat(jnp.concatenate([prior_k, k_here], 0), group, axis=1)
    v_all = jnp.repeat(jnp.concatenate([prior_v, v_here], 0), group, axis=1)
    step_rows = min(256, reach)
    anchor = lax.axis_index("blk") * span
    scale = DH ** (-0.5)

    def one_block(index):
        offset = index * step_rows
        q_block = lax.dynamic_slice_in_dim(q_here, offset, step_rows, 0)
        k_block = lax.dynamic_slice_in_dim(k_all, offset, step_rows + reach, 0)
        v_block = lax.dynamic_slice_in_dim(v_all, offset, step_rows + reach, 0)
        scores = (
            jnp.einsum("qhd,khd->hqk", q_block, k_block, preferred_element_type=jnp.float32) * scale
        )
        q_pos = anchor + offset + jnp.arange(step_rows, dtype=jnp.int32)
        k_pos = anchor + offset - reach + jnp.arange(step_rows + reach, dtype=jnp.int32)
        allowed = (k_pos[None, :] <= q_pos[:, None]) & (k_pos[None, :] > q_pos[:, None] - reach)
        scores = jnp.where(allowed[None], scores, -1e30)
        top = jnp.max(scores, axis=-1, keepdims=True)
        expo = jnp.exp(scores - top)
        weights = (expo / jnp.sum(expo, axis=-1, keepdims=True)).astype(jnp.bfloat16)
        out = jnp.einsum("hqk,khd->qhd", weights, v_block, preferred_element_type=jnp.float32)
        return out.astype(jnp.bfloat16)

    blocks = lax.map(one_block, jnp.arange(span // step_rows, dtype=jnp.int32))
    return blocks.reshape(span, -1)


def average(grad_parts):
    members = lax.axis_size("blk") * lax.axis_size("aa")
    replicas = lax.axis_size("dp")
    flat_grad = grad_parts.reshape(-1)
    share = lax.psum_scatter(flat_grad, ("blk", "aa"), scatter_dimension=0, tiled=True)
    total = lax.psum(share, "dp")
    return total / (members * replicas)


def shards(queries, keys, values, grad_parts):
    attended = attend(queries[0], keys[0], values[0])[None]
    grad_mean = average(grad_parts)
    return (attended, grad_mean)


def fused_kernel(
    sizes, q_hbm, k_hbm, v_hbm, g_hbm, out_ref, mean_ref,
    q_ref, k_ref, v_ref, g_ref, o_send, g1_send, g1_recv, g2_send, g2_recv, g3,
    load_sem, halo_send, halo_recv, o_send_sem, o_recv_sem,
    g1_sem, g2_send_sem, g2_recv_sem, g3_send_sem, g3_recv_sem, far_sem,
):
    n_dp, n_blk, n_aa = sizes
    tok = q_hbm.shape[0]
    reach = tok // 2
    group = HQ // KVH
    kv_here = KVH // n_aa
    wide = group * DH
    n_y = n_blk // 2
    plane = n_y * n_aa
    share = g2_send.shape[1]
    dp, blk, aa = lax.axis_index("dp"), lax.axis_index("blk"), lax.axis_index("aa")
    core, y = blk % 2, blk // 2
    other = 1 - aa
    place = blk * n_aa + aa
    last = n_blk * n_aa - 1
    spot = y * n_aa + aa

    loads = [
        pltpu.make_async_copy(k_hbm, k_ref.at[pl.ds(reach, tok)], load_sem.at[0]),
        pltpu.make_async_copy(v_hbm, v_ref.at[pl.ds(reach, tok)], load_sem.at[1]),
        pltpu.make_async_copy(g_hbm, g_ref, load_sem.at[2]),
        pltpu.make_async_copy(q_hbm, q_ref, load_sem.at[3]),
    ]
    for load in loads:
        load.start()

    partner = (dp, blk + 1 - 2 * core, aa)

    def plane_peer(d):
        to = (spot + d) % plane
        return to, (dp, (to // n_aa) * 2 + core, to % n_aa)

    def dp_peer(d):
        return ((dp + d) % n_dp, blk, aa)

    def at_place(p):
        return (dp, p // n_aa, p % n_aa)

    barrier = pltpu.get_barrier_semaphore()
    greeted = [partner] + [plane_peer(d)[1] for d in range(1, plane)]
    for peer in greeted:
        pl.semaphore_signal(barrier, inc=1, device_id=peer, device_id_type=MESH)
    ahead = (aa == n_aa - 1) & (place < last)
    behind = (aa == 0) & (place > 0)

    @pl.when(dp > 0)
    def _():
        pl.semaphore_signal(barrier, inc=1, device_id=(dp - 1, blk, aa), device_id_type=MESH)

    @pl.when(dp < n_dp - 1)
    def _():
        pl.semaphore_signal(barrier, inc=1, device_id=(dp + 1, blk, aa), device_id_type=MESH)

    @pl.when(ahead)
    def _():
        pl.semaphore_signal(barrier, inc=1, device_id=at_place(place + 1), device_id_type=MESH)

    @pl.when(behind)
    def _():
        pl.semaphore_signal(barrier, inc=1, device_id=at_place(place - 1), device_id_type=MESH)

    @pl.when(place == 0)
    def _():
        k_ref[0:reach] = jnp.zeros((reach, KVH * DH), k_ref.dtype)
        v_ref[0:reach] = jnp.zeros((reach, KVH * DH), v_ref.dtype)

    def rows_of(y_at, core_at):
        return pl.ds(pl.multiple_of((y_at * 2 + core_at) * n_aa * share, share), n_aa * share)

    loads[2].wait()
    for y_at in range(n_y):
        g1_send[y_at] = g_ref[rows_of(y_at, 1 - core)].astype(jnp.bfloat16)
    loads[0].wait()
    loads[1].wait()

    extra = [ahead | behind, dp > 0, dp < n_dp - 1]
    pl.semaphore_wait(barrier, len(greeted) + sum(e.astype(jnp.int32) for e in extra))

    def tell(k):
        @pl.when((dp > 0) & (dp + 1 + k < n_dp))
        def _():
            pl.semaphore_signal(
                far_sem.at[0, k], inc=1, device_id=(dp - 1, blk, aa), device_id_type=MESH
            )

        @pl.when((dp < n_dp - 1) & (dp - 1 - k >= 0))
        def _():
            pl.semaphore_signal(
                far_sem.at[1, k], inc=1, device_id=(dp + 1, blk, aa), device_id_type=MESH
            )

    def hear(k):
        @pl.when(dp + 2 + k < n_dp)
        def _():
            pl.semaphore_wait(far_sem.at[0, k], 1)

        @pl.when(dp - 2 - k >= 0)
        def _():
            pl.semaphore_wait(far_sem.at[1, k], 1)

    def remote(src, dst, send_sem, recv_sem, to):
        return pltpu.make_async_remote_copy(
            src_ref=src, dst_ref=dst, send_sem=send_sem, recv_sem=recv_sem,
            device_id=to, device_id_type=MESH,
        )

    first = remote(g1_send, g1_recv, g1_sem.at[0], g1_sem.at[1], partner)
    first.start()
    if n_dp > 2:
        tell(0)

    def halo(ref, i):
        return remote(
            ref.at[pl.ds(tok, reach)], ref.at[pl.ds(0, reach)],
            halo_send.at[i], halo_recv.at[i], at_place(jnp.minimum(place + 1, last)),
        )

    @pl.when(place < last)
    def _():
        halo(k_ref, 0).start()
        halo(v_ref, 1).start()

    def unit(block, kv, target):
        kv_at = target * kv_here + kv
        rows = pl.ds(block * reach, reach)
        span = pl.ds(block * reach, 2 * reach)
        q_cols = pl.multiple_of(kv_at * wide, wide)
        kv_cols = pl.ds(pl.multiple_of(kv_at * DH, DH), DH)
        q_all = q_ref[rows, pl.ds(q_cols, wide)]
        q = jnp.concatenate([q_all[:, h * DH : (h + 1) * DH] for h in range(group)], 0)
        scores = lax.dot_general(
            q, k_ref[span, kv_cols], (((1,), (1,)), ((), ())), preferred_element_type=jnp.float32
        ) * (DH ** -0.5)
        i = lax.broadcasted_iota(jnp.int32, scores.shape, 0) % reach
        j = lax.broadcasted_iota(jnp.int32, scores.shape, 1)
        scores = jnp.where((j > i) & (j <= i + reach), scores, -1e30)
        expo = jnp.exp(scores - jnp.max(scores, axis=-1, keepdims=True))
        weights = (expo / jnp.sum(expo, axis=-1, keepdims=True)).astype(jnp.bfloat16)
        out = jnp.dot(weights, v_ref[span, kv_cols], preferred_element_type=jnp.float32)
        out = out.astype(jnp.bfloat16)
        return jnp.concatenate([out[h * reach : (h + 1) * reach] for h in range(group)], 1)

    def send_out(block, kv):
        cols = pl.ds(kv * wide, wide)
        start = pl.multiple_of(aa * tok + block * reach, reach)
        at = block * kv_here + kv
        return remote(
            o_send.at[pl.ds(block * reach, reach), cols], out_ref.at[pl.ds(start, reach), cols],
            o_send_sem.at[at], o_recv_sem.at[at], (dp, blk, other),
        )

    def for_other(block):
        for kv in range(kv_here):
            o_send[pl.ds(block * reach, reach), pl.ds(kv * wide, wide)] = unit(block, kv, other)

    def for_self(block):
        for kv in range(kv_here):
            start = pl.multiple_of(aa * tok + block * reach, reach)
            out_ref[pl.ds(start, reach), pl.ds(kv * wide, wide)] = unit(block, kv, aa)

    loads[3].wait()
    for_other(1)

    first.wait_recv()
    for y_at in range(n_y):
        summed = g_ref[rows_of(y_at, core)] + g1_recv[y_at].astype(jnp.float32)
        for a_at in range(n_aa):
            g2_send[y_at * n_aa + a_at] = summed[a_at * share : (a_at + 1) * share].astype(jnp.bfloat16)

    def second(d):
        to, peer = plane_peer(d)
        return remote(
            g2_send.at[to], g2_recv.at[d - 1], g2_send_sem.at[d - 1], g2_recv_sem.at[d - 1], peer
        )

    for d in range(1, plane):
        second(d).start()
    for kv in range(kv_here):
        send_out(1, kv).start()
    for_self(1)
    for k in range(1, n_dp - 2):
        hear(k - 1)
        tell(k)

    @pl.when(place > 0)
    def _():
        halo(k_ref, 0).wait_recv()
        halo(v_ref, 1).wait_recv()

    for_other(0)
    for kv in range(kv_here):
        send_out(0, kv).start()

    own_rows = pl.ds(pl.multiple_of(place * share, share), share)
    own = g_ref[own_rows] + g1_recv[y, pl.ds(pl.multiple_of(aa * share, share), share)].astype(jnp.float32)
    for d in range(1, plane):
        second(d).wait_recv()
        own = own + g2_recv[d - 1].astype(jnp.float32)
    g3[dp] = own.astype(jnp.bfloat16)

    def third(d):
        return remote(
            g3.at[dp], g3.at[dp], g3_send_sem.at[d - 1], g3_recv_sem.at[d - 1], dp_peer(d)
        )

    def third_in(d):
        origin = (dp + n_dp - d) % n_dp
        return remote(
            g3.at[origin], g3.at[origin], g3_send_sem.at[d - 1], g3_recv_sem.at[d - 1], dp_peer(d)
        )

    if n_dp > 2:
        hear(n_dp - 3)
    for d in range(1, n_dp):
        third(d).start()

    for_self(0)
    for d in range(1, n_dp):
        third_in(d).wait_recv()
    total = g3[0].astype(jnp.float32)
    for z in range(1, n_dp):
        total = total + g3[z].astype(jnp.float32)
    mean_ref[...] = total / (n_dp * n_blk * n_aa)

    first.wait_send()

    @pl.when(place < last)
    def _():
        halo(k_ref, 0).wait_send()
        halo(v_ref, 1).wait_send()

    for d in range(1, plane):
        second(d).wait_send()
    for d in range(1, n_dp):
        third(d).wait_send()
    for block in (1, 0):
        for kv in range(kv_here):
            send_out(block, kv).wait()


def finish_kernel(out_in, mean_in, out_ref, mean_ref, sem):
    out_copy = pltpu.make_async_copy(out_in, out_ref, sem.at[0])
    mean_copy = pltpu.make_async_copy(mean_in, mean_ref, sem.at[1])
    out_copy.start()
    mean_copy.start()
    out_copy.wait()
    mean_copy.wait()


def fused(sizes, queries, keys, values, grad_parts):
    n_dp, n_blk, n_aa = sizes
    tok, q_width = queries.shape[1:]
    reach = tok // 2
    rows = grad_parts.size // LANES
    share = rows // (n_blk * n_aa)
    plane = n_blk // 2 * n_aa
    kv_here = KVH // n_aa
    bf16, f32 = jnp.bfloat16, jnp.float32
    dma = lambda *shape: pltpu.SemaphoreType.DMA(shape)
    vmem = pl.BlockSpec(memory_space=pltpu.VMEM)
    hbm = pl.BlockSpec(memory_space=pl.ANY)
    attended, mean = pl.pallas_call(
        functools.partial(fused_kernel, sizes),
        out_shape=(
            pltpu.VMEM((tok * n_aa, q_width // n_aa), bf16),
            pltpu.VMEM((share, LANES), f32),
        ),
        in_specs=[hbm] * 4,
        out_specs=(vmem, vmem),
        scratch_shapes=[
            pltpu.VMEM((tok, q_width), bf16),
            pltpu.VMEM((reach + tok, KVH * DH), bf16),
            pltpu.VMEM((reach + tok, KVH * DH), bf16),
            pltpu.VMEM((rows, LANES), f32),
            pltpu.VMEM((tok, q_width // n_aa), bf16),
            pltpu.VMEM((n_blk // 2, n_aa * share, LANES), bf16),
            pltpu.VMEM((n_blk // 2, n_aa * share, LANES), bf16),
            pltpu.VMEM((plane, share, LANES), bf16),
            pltpu.VMEM((plane - 1, share, LANES), bf16),
            pltpu.VMEM((n_dp, share, LANES), bf16),
            dma(4), dma(2), dma(2), dma(2 * kv_here), dma(2 * kv_here),
            dma(2), dma(plane - 1), dma(plane - 1), dma(n_dp - 1), dma(n_dp - 1),
            pltpu.SemaphoreType.REGULAR((2, max(n_dp - 2, 1))),
        ],
        compiler_params=pltpu.CompilerParams(collective_id=0, has_side_effects=True),
        name="fused",
    )(queries[0], keys[0], values[0], grad_parts.reshape(rows, LANES))
    attended, mean = pl.pallas_call(
        finish_kernel,
        out_shape=tuple(jax.ShapeDtypeStruct(a.shape, a.dtype) for a in (attended, mean)),
        in_specs=[hbm] * 2,
        out_specs=(hbm, hbm),
        scratch_shapes=[dma(2)],
        compiler_params=pltpu.CompilerParams(vmem_limit_bytes=1024 * 1024),
        name="finish",
    )(attended, mean)
    return attended[None], mean.reshape(-1)


def fits(sizes, args):
    n_dp, n_blk, n_aa = sizes
    queries, _, _, grad_parts = args
    rows, rest = divmod(grad_parts.shape[-1], LANES)
    shares = n_blk * n_aa
    tokens = queries.shape[1] // shares
    return (
        n_aa == 2 and n_blk % 2 == 0 and n_dp > 1 and KVH % n_aa == 0
        and tokens % 32 == 0 and rest == 0 and rows % (shares * 16) == 0
    )


def solution(mesh):
    placed = (
        P("dp", ("blk", "aa"), None),
        P("dp", ("blk", "aa"), None),
        P("dp", ("blk", "aa"), None),
        P("dp", ("blk", "aa"), None),
    )
    sizes = tuple(mesh.shape[axis] for axis in ("dp", "blk", "aa"))

    def step(*args):
        body = functools.partial(fused, sizes) if fits(sizes, args) else shards
        return jax.shard_map(
            body,
            mesh=mesh,
            in_specs=placed,
            out_specs=(P("dp", "blk", "aa"), P(("blk", "aa"))),
            check_vma=False,
        )(*args)

    return step
```
